32 devices in a mesh: gx: 16 (over z, y, x), gy: 1, gz: 2 (over core).
Axes of the slice: x: 2, y: 2, z: 4, core: 2. Of those that a mesh axis runs over, the one named last changes fastest.
Arguments:
- populations: float32 [19, 128, 8, 256], P(None, 'gx', 'gy', 'gz'), may hold values from 0.01 to 0.11
Outputs:
- populations_next: float32 [19, 128, 8, 256], P(None, 'gx', 'gy', 'gz')
- moments_slab: float32 [4, 256, 8, 128], P(None, ('gz', 'gx'), 'gy')
The draws below stay inside these ranges and needn't reach their ends.
All inputs are finite; a program needn't handle non-finite values.
Results may differ from the reference program's by a relative error of at most 0.0003.
Values sent between devices are 32-bit elements; how exact they have to be, the bound alone decides.
A program may use at most 64 MiB of HBM per device.

```python
from functools import reduce
import jax
import jax.numpy as jnp

Q = 19
NX = 128
NY = 8
NZ = 256


def levels(key, dims, cuts, least, largest):
    loudness = 1.0
    for position, parts in cuts:
        heights = jax.random.uniform(jax.random.fold_in(jax.random.fold_in(key, 6), position), (parts,), jnp.float32, least / len(cuts), largest / len(cuts))
        loudness = loudness * jnp.repeat(jnp.exp(heights), dims[position] // parts).reshape((-1,) + (1,) * (len(dims) - 1 - position))
    return loudness


def setup_inputs(seed: int = 0) -> dict:
    seeds = jax.random.split(jax.random.key(seed), 2)
    populations = jnp.clip(0.01 + 0.1 * jax.random.uniform(seeds[0], (Q, NX, NY, NZ), jnp.float32) ** levels(seeds[0], (Q, NX, NY, NZ), ((1, 16), (3, 2)), -0.2, 0.2), 0.01, 0.11)
    return dict(populations=populations)


lattice_moves = [(0, 0, 0), (1, 0, 0), (-1, 0, 0), (0, 1, 0), (0, -1, 0), (0, 0, 1), (0, 0, -1),
                 (1, 1, 0), (-1, -1, 0), (1, -1, 0), (-1, 1, 0), (1, 0, 1), (-1, 0, -1), (1, 0, -1), (-1, 0, 1),
                 (0, 1, 1), (0, -1, -1), (0, 1, -1), (0, -1, 1)]
lattice_weights = [1.0 / 3.0] + [1.0 / 18.0] * 6 + [1.0 / 36.0] * 12
relaxation = 1.6


def signed_total(pieces, component):
    total = jnp.zeros_like(pieces[0])
    for move, piece in zip(lattice_moves, pieces):
        if move[component] == 1:
            total = total + piece
        elif move[component] == -1:
            total = total - piece
    return total


def lattice_moments(pieces):
    density = reduce(lambda left, right: left + right, pieces)
    velocity_x = signed_total(pieces, 0) / density
    velocity_y = signed_total(pieces, 1) / density
    velocity_z = signed_total(pieces, 2) / density
    return density, velocity_x, velocity_y, velocity_z


def collide(pieces):
    density, velocity_x, velocity_y, velocity_z = lattice_moments(pieces)
    speed_sq = velocity_x * velocity_x + velocity_y * velocity_y + velocity_z * velocity_z
    result = []
    for move, weight, piece in zip(lattice_moves, lattice_weights, pieces):
        projected = move[0] * velocity_x + move[1] * velocity_y + move[2] * velocity_z
        balance = weight * density * (1.0 + 3.0 * projected + 4.5 * projected * projected - 1.5 * speed_sq)
        result.append(piece - relaxation * (piece - balance))
    return result


def reference(populations):
    pieces = [populations[index] for index in range(19)]
    moments = jnp.stack(lattice_moments(pieces))
    moments_slab = jnp.transpose(moments, (0, 3, 2, 1))
    read = [jnp.roll(pieces[index], lattice_moves[index], axis=(0, 1, 2)) for index in range(19)]
    populations_next = jnp.stack(collide(read))
    return populations_next, moments_slab
```

```python
import functools

import jax
import jax.numpy as jnp
from jax import lax
from jax.experimental import pallas as pl
from jax.experimental.pallas import tpu as pltpu
from jax.sharding import PartitionSpec as P

MESH = pl.DeviceIdType.MESH

lattice_moves = [
    (0, 0, 0),
    (1, 0, 0),
    (-1, 0, 0),
    (0, 1, 0),
    (0, -1, 0),
    (0, 0, 1),
    (0, 0, -1),
    (1, 1, 0),
    (-1, -1, 0),
    (1, -1, 0),
    (-1, 1, 0),
    (1, 0, 1),
    (-1, 0, -1),
    (1, 0, -1),
    (-1, 0, 1),
    (0, 1, 1),
    (0, -1, -1),
    (0, 1, -1),
    (0, -1, 1),
]
lattice_weights = [1.0 / 3.0] + [1.0 / 18.0] * 6 + [1.0 / 36.0] * 12
relaxation = 1.6
count_q = len(lattice_moves)


def movers(component, sign):
    return [q for q, move in enumerate(lattice_moves) if move[component] == sign]


def place_in(q, component):
    return movers(component, lattice_moves[q][component]).index(q)


def side(sign):
    return 0 if sign > 0 else 1


edges_xz = [q for q, m in enumerate(lattice_moves) if m[0] and m[2]]
edges_xy = [q for q, m in enumerate(lattice_moves) if m[0] and m[1]]
edges_yz = [q for q, m in enumerate(lattice_moves) if m[1] and m[2]]


def total(terms):
    terms = list(terms)
    while len(terms) > 1:
        terms = [
            terms[i] + terms[i + 1] if i + 1 < len(terms) else terms[i]
            for i in range(0, len(terms), 2)
        ]
    return terms[0]


def moments_of(f):
    density = total(f)
    inverse = 1.0 / density
    velocity = []
    for component in range(3):
        plus = total(f[q] for q in movers(component, 1))
        minus = total(f[q] for q in movers(component, -1))
        velocity.append((plus - minus) * inverse)
    return density, velocity


def collided(f):
    density, velocity = moments_of(f)
    speed_sq = velocity[0] * velocity[0] + velocity[1] * velocity[1] + velocity[2] * velocity[2]
    base = 1.0 - 1.5 * speed_sq
    scaled = {w: (relaxation * w) * density for w in set(lattice_weights)}
    keep = 1.0 - relaxation
    result = [None] * count_q
    result[0] = keep * f[0] + scaled[lattice_weights[0]] * base
    for q in range(1, count_q, 2):
        move = lattice_moves[q]
        projected = None
        for component in range(3):
            if move[component] == 0:
                continue
            if projected is None:
                projected = velocity[component] if move[component] > 0 else -velocity[component]
            elif move[component] > 0:
                projected = projected + velocity[component]
            else:
                projected = projected - velocity[component]
        even = base + 4.5 * (projected * projected)
        odd = 3.0 * projected
        weight = scaled[lattice_weights[q]]
        result[q] = keep * f[q] + weight * (even + odd)
        result[q + 1] = keep * f[q + 1] + weight * (even - odd)
    return result


def rolled(v, shift, axis):
    return pltpu.roll(v, shift % v.shape[axis], axis)


def kernel(axes, sizes, pop_hbm, next_ref, slab_ref,
           pop, out_vm, slab_vm, face_x, edge_xz, pack_z, face_z, send_m, recv_m, mid,
           row_y, face_y, edge_xy, edge_yz,
           load_sem, store_sem, send_sem, recv_sem, send_m_sem, recv_m_sem):
    nx, ny, nz = (sizes[a] for a in axes)
    here = tuple(lax.axis_index(a) for a in axes)
    _, lx, ly, lz = pop.shape
    split_y = ny > 1

    def device_at(offset):
        return tuple(
            lax.rem(h + (o % n), n) if o % n else h
            for h, o, n in zip(here, offset, (nx, ny, nz))
        )

    offsets = [(k, 0, 0) for k in range(1, nx)]
    offsets += [(0, 0, 1), (0, 0, -1)]
    offsets += [lattice_moves[q] for q in edges_xz]
    if split_y:
        offsets += [(0, 1, 0), (0, -1, 0)]
        offsets += [lattice_moves[q] for q in edges_xy + edges_yz]
    partners = sorted({(a % nx, b % ny, c % nz) for a, b, c in offsets})
    barrier = pltpu.get_barrier_semaphore()
    for offset in partners:
        pl.semaphore_signal(barrier, inc=1, device_id=device_at(offset), device_id_type=MESH)

    load = pltpu.make_async_copy(pop_hbm, pop, load_sem)
    load.start()
    load.wait()

    lane = lax.broadcasted_iota(jnp.int32, (ly, lz), 1)
    row = lax.broadcasted_iota(jnp.int32, (ly, lz), 0)

    for sign in (1, -1):
        at = lz - 1 if sign > 0 else 0
        packed = jnp.zeros((ly, lz), jnp.float32)
        for i, q in enumerate(movers(2, sign)):
            for x in range(lx):
                k = i * lx + x
                packed = jnp.where(lane == k, rolled(pop[q, x], k - at, 1), packed)
        pack_z[side(sign)] = packed
    if split_y:
        for sign in (1, -1):
            at = ly - 1 if sign > 0 else 0
            for i, q in enumerate(movers(1, sign)):
                for x in range(lx):
                    row_y[side(sign), i, x:x + 1, :] = pop[q, x, at:at + 1, :]

    values = [[None] * lx for _ in range(4)]
    for x in range(lx):
        density, velocity = moments_of([pop[q, x] for q in range(count_q)])
        for c, v in enumerate([density] + velocity):
            values[c][x] = v
    for c in range(4):
        tiles = values[c]
        step = 1
        while step < lx:
            upper = (lane & step) != 0
            fresh = list(tiles)
            for x in range(lx):
                if x & step:
                    continue
                a, b = tiles[x], tiles[x + step]
                fresh[x] = jnp.where(upper, rolled(b, step, 1), a)
                fresh[x + step] = jnp.where(upper, b, rolled(a, -step, 1))
            tiles = fresh
            step *= 2
        for z in range(lx):
            mid[c, z * ly:(z + 1) * ly, :] = tiles[z]
    for p in range(2):
        square = mid[2 * p:2 * p + 2].reshape(lz, lz).T
        for j in range(nx):
            send_m[j, p] = square[j * lx:(j + 1) * lx]

    pl.semaphore_wait(barrier, len(partners))

    me = here[0]
    outgoing = []
    count = [0]

    def send(src, dst, offset):
        s = count[0]
        count[0] += 1
        copy = pltpu.make_async_remote_copy(
            src_ref=src, dst_ref=dst, send_sem=send_sem.at[s], recv_sem=recv_sem.at[s],
            device_id=device_at(offset), device_id_type=MESH)
        copy.start()
        outgoing.append(copy)
        return copy

    moment_copies = []

    def send_moments(k):
        target = device_at((k, 0, 0))
        copy = pltpu.make_async_remote_copy(
            src_ref=send_m.at[target[0]], dst_ref=recv_m.at[me],
            send_sem=send_m_sem.at[k], recv_sem=recv_m_sem.at[k],
            device_id=target, device_id_type=MESH)
        copy.start()
        moment_copies.append(copy)

    z_copies, x_copies = [], []
    for sign in (1, -1):
        s = side(sign)
        z_copies.append(send(pack_z.at[s], face_z.at[s], (0, 0, sign)))
    for sign in (1, -1):
        s, at = side(sign), lx - 1 if sign > 0 else 0
        for i, q in enumerate(movers(0, sign)):
            x_copies.append(send(pop.at[q, at], face_x.at[s, i], (sign, 0, 0)))
    for i, q in enumerate(edges_xz):
        at = lx - 1 if lattice_moves[q][0] > 0 else 0
        x_copies.append(send(pop.at[q, at], edge_xz.at[i], lattice_moves[q]))
    if split_y:
        for sign in (1, -1):
            s = side(sign)
            z_copies.append(send(row_y.at[s], face_y.at[s], (0, sign, 0)))
        for i, q in enumerate(edges_yz):
            s = side(lattice_moves[q][2])
            z_copies.append(send(pack_z.at[s], edge_yz.at[i], lattice_moves[q]))
        for i, q in enumerate(edges_xy):
            s = side(lattice_moves[q][1])
            x_copies.append(send(row_y.at[s, place_in(q, 1)], edge_xy.at[i], lattice_moves[q]))
    for k in sorted(range(1, nx), key=lambda k: abs(k - nx // 2)):
        send_moments(k)
    recv_m[me] = send_m[me]

    def streamed(q, x):
        cx, cy, cz = lattice_moves[q]
        sx = x - cx
        inside = 0 <= sx < lx
        sx_wrapped = sx % lx
        v = pop[q, sx] if inside else face_x[side(cx), place_in(q, 0)]
        if cy and split_y:
            at = ly - 1 if cy > 0 else 0
            if inside:
                other = face_y[side(cy), place_in(q, 1), sx:sx + 1, :]
            else:
                other = edge_xy[edges_xy.index(q), sx_wrapped:sx_wrapped + 1, :]
            v = jnp.where(row == at, jnp.broadcast_to(other, v.shape), v)
        if cz:
            at = lz - 1 if cz > 0 else 0
            if inside:
                other = face_z[side(cz)]
                if cy and split_y:
                    at_y = ly - 1 if cy > 0 else 0
                    other = jnp.where(row == at_y, edge_yz[edges_yz.index(q)], other)
                k = place_in(q, 2) * lx + sx
                other = rolled(other, at - k, 1)
            else:
                other = edge_xz[edges_xz.index(q)]
            v = jnp.where(lane == at, other, v)
        if cy:
            v = rolled(v, cy, 0)
        if cz:
            v = rolled(v, cz, 1)
        return v

    def advance(x):
        result = collided([streamed(q, x) for q in range(count_q)])
        for q in range(count_q):
            out_vm[q, x] = result[q]

    for copy in z_copies:
        copy.wait_recv()
    for x in range(1, lx - 1):
        advance(x)
    for copy in x_copies:
        copy.wait_recv()
    advance(0)
    advance(lx - 1)
    store_next = pltpu.make_async_copy(out_vm, next_ref, store_sem.at[0])
    store_next.start()

    for copy in moment_copies:
        copy.wait_recv()
    for p in range(2):
        square = recv_m[:, p].reshape(lz, lz).T
        slab_vm[2 * p:2 * p + 2] = square.reshape(2, lx, ly, lz)
    store_slab = pltpu.make_async_copy(slab_vm, slab_ref, store_sem.at[1])
    store_slab.start()
    for copy in outgoing + moment_copies:
        copy.wait_send()
    store_next.wait()
    store_slab.wait()


def on_device(axes, sizes, populations):
    q, lx, ly, lz = populations.shape
    nx = sizes[axes[0]]
    messages = 2 + 10 + 4
    if sizes[axes[1]] > 1:
        messages += 2 + 4 + 4
    f32 = jnp.float32
    tile = (ly, lz)
    return pl.pallas_call(
        functools.partial(kernel, axes, sizes),
        out_shape=(
            jax.ShapeDtypeStruct(populations.shape, f32),
            jax.ShapeDtypeStruct((4, lz // nx, ly, lx * nx), f32),
        ),
        in_specs=[pl.BlockSpec(memory_space=pl.ANY)],
        out_specs=(pl.BlockSpec(memory_space=pl.ANY),) * 2,
        scratch_shapes=[
            pltpu.VMEM(populations.shape, f32),
            pltpu.VMEM(populations.shape, f32),
            pltpu.VMEM((4, lz // nx, ly, lx * nx), f32),
            pltpu.VMEM((2, 5) + tile, f32),
            pltpu.VMEM((4,) + tile, f32),
            pltpu.VMEM((2,) + tile, f32),
            pltpu.VMEM((2,) + tile, f32),
            pltpu.VMEM((nx, 2, lx, lz), f32),
            pltpu.VMEM((nx, 2, lx, lz), f32),
            pltpu.VMEM((4, lx * ly, lz), f32),
            pltpu.VMEM((2, 5, lx, lz), f32),
            pltpu.VMEM((2, 5, lx, lz), f32),
            pltpu.VMEM((4, lx, lz), f32),
            pltpu.VMEM((4,) + tile, f32),
            pltpu.SemaphoreType.DMA,
            pltpu.SemaphoreType.DMA((2,)),
            pltpu.SemaphoreType.DMA((messages,)),
            pltpu.SemaphoreType.DMA((messages,)),
            pltpu.SemaphoreType.DMA((nx,)),
            pltpu.SemaphoreType.DMA((nx,)),
        ],
        compiler_params=pltpu.CompilerParams(collective_id=0, has_side_effects=True),
        name="lattice_step",
    )(populations)


def solution(mesh):
    axes = tuple(mesh.axis_names)
    sizes = dict(mesh.shape)
    return jax.shard_map(
        functools.partial(on_device, axes, sizes),
        mesh=mesh,
        in_specs=(P(None, "gx", "gy", "gz"),),
        out_specs=(P(None, "gx", "gy", "gz"), P(None, ("gz", "gx"), "gy", None)),
        check_vma=False,
    )
```

```python
import functools

import jax
import jax.numpy as jnp
from jax import lax
from jax.experimental import pallas as pl
from jax.experimental.pallas import tpu as pltpu
from jax.sharding import PartitionSpec as P

MESH = pl.DeviceIdType.MESH

lattice_moves = [
    (0, 0, 0),
    (1, 0, 0),
    (-1, 0, 0),
    (0, 1, 0),
    (0, -1, 0),
    (0, 0, 1),
    (0, 0, -1),
    (1, 1, 0),
    (-1, -1, 0),
    (1, -1, 0),
    (-1, 1, 0),
    (1, 0, 1),
    (-1, 0, -1),
    (1, 0, -1),
    (-1, 0, 1),
    (0, 1, 1),
    (0, -1, -1),
    (0, 1, -1),
    (0, -1, 1),
]
lattice_weights = [1.0 / 3.0] + [1.0 / 18.0] * 6 + [1.0 / 36.0] * 12
relaxation = 1.6
count_q = len(lattice_moves)


def movers(component, sign):
    return [q for q, move in enumerate(lattice_moves) if move[component] == sign]


def place_in(q, component):
    return movers(component, lattice_moves[q][component]).index(q)


def side(sign):
    return 0 if sign > 0 else 1


edges_xz = [q for q, m in enumerate(lattice_moves) if m[0] and m[2]]
edges_xy = [q for q, m in enumerate(lattice_moves) if m[0] and m[1]]
edges_yz = [q for q, m in enumerate(lattice_moves) if m[1] and m[2]]


def total(terms):
    terms = list(terms)
    while len(terms) > 1:
        terms = [
            terms[i] + terms[i + 1] if i + 1 < len(terms) else terms[i]
            for i in range(0, len(terms), 2)
        ]
    return terms[0]


def moments_of(f):
    density = total(f)
    inverse = 1.0 / density
    velocity = []
    for component in range(3):
        plus = total(f[q] for q in movers(component, 1))
        minus = total(f[q] for q in movers(component, -1))
        velocity.append((plus - minus) * inverse)
    return density, velocity


def collided(f):
    density, velocity = moments_of(f)
    speed_sq = velocity[0] * velocity[0] + velocity[1] * velocity[1] + velocity[2] * velocity[2]
    base = 1.0 - 1.5 * speed_sq
    scaled = {w: (relaxation * w) * density for w in set(lattice_weights)}
    keep = 1.0 - relaxation
    result = [None] * count_q
    result[0] = keep * f[0] + scaled[lattice_weights[0]] * base
    for q in range(1, count_q, 2):
        move = lattice_moves[q]
        projected = None
        for component in range(3):
            if move[component] == 0:
                continue
            if projected is None:
                projected = velocity[component] if move[component] > 0 else -velocity[component]
            elif move[component] > 0:
                projected = projected + velocity[component]
            else:
                projected = projected - velocity[component]
        even = base + 4.5 * (projected * projected)
        odd = 3.0 * projected
        weight = scaled[lattice_weights[q]]
        result[q] = keep * f[q] + weight * (even + odd)
        result[q + 1] = keep * f[q + 1] + weight * (even - odd)
    return result


def rolled(v, shift, axis):
    return pltpu.roll(v, shift % v.shape[axis], axis)


def kernel(axes, sizes, pop_hbm, out_vm, slab_vm,
           pop, face_x, edge_xz, pack_z, face_z, send_m, recv_m, mid,
           row_y, face_y, edge_xy, edge_yz,
           load_sem, send_sem, recv_sem, send_m_sem, recv_m_sem):
    nx, ny, nz = (sizes[a] for a in axes)
    here = tuple(lax.axis_index(a) for a in axes)
    _, lx, ly, lz = pop.shape
    split_y = ny > 1

    def device_at(offset):
        return tuple(
            lax.rem(h + (o % n), n) if o % n else h
            for h, o, n in zip(here, offset, (nx, ny, nz))
        )

    offsets = [(k, 0, 0) for k in range(1, nx)]
    offsets += [(0, 0, 1), (0, 0, -1)]
    offsets += [lattice_moves[q] for q in edges_xz]
    if split_y:
        offsets += [(0, 1, 0), (0, -1, 0)]
        offsets += [lattice_moves[q] for q in edges_xy + edges_yz]
    partners = sorted({(a % nx, b % ny, c % nz) for a, b, c in offsets})
    barrier = pltpu.get_barrier_semaphore()
    for offset in partners:
        pl.semaphore_signal(barrier, inc=1, device_id=device_at(offset), device_id_type=MESH)

    load = pltpu.make_async_copy(pop_hbm, pop, load_sem)
    load.start()
    load.wait()

    lane = lax.broadcasted_iota(jnp.int32, (ly, lz), 1)
    row = lax.broadcasted_iota(jnp.int32, (ly, lz), 0)

    for sign in (1, -1):
        at = lz - 1 if sign > 0 else 0
        packed = jnp.zeros((ly, lz), jnp.float32)
        for i, q in enumerate(movers(2, sign)):
            for x in range(lx):
                k = i * lx + x
                packed = jnp.where(lane == k, rolled(pop[q, x], k - at, 1), packed)
        pack_z[side(sign)] = packed
    if split_y:
        for sign in (1, -1):
            at = ly - 1 if sign > 0 else 0
            for i, q in enumerate(movers(1, sign)):
                for x in range(lx):
                    row_y[side(sign), i, x:x + 1, :] = pop[q, x, at:at + 1, :]

    values = [[None] * lx for _ in range(4)]
    for x in range(lx):
        density, velocity = moments_of([pop[q, x] for q in range(count_q)])
        for c, v in enumerate([density] + velocity):
            values[c][x] = v
    for c in range(4):
        tiles = values[c]
        step = 1
        while step < lx:
            upper = (lane & step) != 0
            fresh = list(tiles)
            for x in range(lx):
                if x & step:
                    continue
                a, b = tiles[x], tiles[x + step]
                fresh[x] = jnp.where(upper, rolled(b, step, 1), a)
                fresh[x + step] = jnp.where(upper, b, rolled(a, -step, 1))
            tiles = fresh
            step *= 2
        for z in range(lx):
            mid[c, z * ly:(z + 1) * ly, :] = tiles[z]
    for p in range(2):
        square = mid[2 * p:2 * p + 2].reshape(lz, lz).T
        for j in range(nx):
            send_m[j, p] = square[j * lx:(j + 1) * lx]

    pl.semaphore_wait(barrier, len(partners))

    me = here[0]
    outgoing = []
    count = [0]

    def send(src, dst, offset):
        s = count[0]
        count[0] += 1
        copy = pltpu.make_async_remote_copy(
            src_ref=src, dst_ref=dst, send_sem=send_sem.at[s], recv_sem=recv_sem.at[s],
            device_id=device_at(offset), device_id_type=MESH)
        copy.start()
        outgoing.append(copy)
        return copy

    moment_copies = []

    def send_moments(k):
        target = device_at((k, 0, 0))
        copy = pltpu.make_async_remote_copy(
            src_ref=send_m.at[target[0]], dst_ref=recv_m.at[me],
            send_sem=send_m_sem.at[k], recv_sem=recv_m_sem.at[k],
            device_id=target, device_id_type=MESH)
        copy.start()
        moment_copies.append(copy)

    z_copies, x_copies = [], []
    for sign in (1, -1):
        s = side(sign)
        z_copies.append(send(pack_z.at[s], face_z.at[s], (0, 0, sign)))
    for sign in (1, -1):
        s, at = side(sign), lx - 1 if sign > 0 else 0
        for i, q in enumerate(movers(0, sign)):
            x_copies.append(send(pop.at[q, at], face_x.at[s, i], (sign, 0, 0)))
    for i, q in enumerate(edges_xz):
        at = lx - 1 if lattice_moves[q][0] > 0 else 0
        x_copies.append(send(pop.at[q, at], edge_xz.at[i], lattice_moves[q]))
    if split_y:
        for sign in (1, -1):
            s = side(sign)
            z_copies.append(send(row_y.at[s], face_y.at[s], (0, sign, 0)))
        for i, q in enumerate(edges_yz):
            s = side(lattice_moves[q][2])
            z_copies.append(send(pack_z.at[s], edge_yz.at[i], lattice_moves[q]))
        for i, q in enumerate(edges_xy):
            s = side(lattice_moves[q][1])
            x_copies.append(send(row_y.at[s, place_in(q, 1)], edge_xy.at[i], lattice_moves[q]))
    for k in sorted(range(1, nx), key=lambda k: abs(k - nx // 2)):
        send_moments(k)
    recv_m[me] = send_m[me]

    def streamed(q, x):
        cx, cy, cz = lattice_moves[q]
        sx = x - cx
        inside = 0 <= sx < lx
        sx_wrapped = sx % lx
        v = pop[q, sx] if inside else face_x[side(cx), place_in(q, 0)]
        if cy and split_y:
            at = ly - 1 if cy > 0 else 0
            if inside:
                other = face_y[side(cy), place_in(q, 1), sx:sx + 1, :]
            else:
                other = edge_xy[edges_xy.index(q), sx_wrapped:sx_wrapped + 1, :]
            v = jnp.where(row == at, jnp.broadcast_to(other, v.shape), v)
        if cz:
            at = lz - 1 if cz > 0 else 0
            if inside:
                other = face_z[side(cz)]
                if cy and split_y:
                    at_y = ly - 1 if cy > 0 else 0
                    other = jnp.where(row == at_y, edge_yz[edges_yz.index(q)], other)
                k = place_in(q, 2) * lx + sx
                other = rolled(other, at - k, 1)
            else:
                other = edge_xz[edges_xz.index(q)]
            v = jnp.where(lane == at, other, v)
        if cy:
            v = rolled(v, cy, 0)
        if cz:
            v = rolled(v, cz, 1)
        return v

    def advance(x):
        result = collided([streamed(q, x) for q in range(count_q)])
        for q in range(count_q):
            out_vm[q, x] = result[q]

    for copy in z_copies:
        copy.wait_recv()
    for x in range(1, lx - 1):
        advance(x)
    for copy in x_copies:
        copy.wait_recv()
    advance(0)
    advance(lx - 1)

    for copy in moment_copies:
        copy.wait_recv()
    for p in range(2):
        square = recv_m[:, p].reshape(lz, lz).T
        slab_vm[2 * p:2 * p + 2] = square.reshape(2, lx, ly, lz)
    for copy in outgoing + moment_copies:
        copy.wait_send()


def write_out(next_vm, slab_vm, next_ref, slab_ref, sems):
    stores = [
        pltpu.make_async_copy(next_vm, next_ref, sems.at[0]),
        pltpu.make_async_copy(slab_vm, slab_ref, sems.at[1]),
    ]
    for store in stores:
        store.start()
    for store in stores:
        store.wait()


def on_device(axes, sizes, populations):
    q, lx, ly, lz = populations.shape
    nx = sizes[axes[0]]
    messages = 2 + 10 + 4
    if sizes[axes[1]] > 1:
        messages += 2 + 4 + 4
    f32 = jnp.float32
    tile = (ly, lz)
    held = pl.pallas_call(
        functools.partial(kernel, axes, sizes),
        out_shape=(
            pltpu.VMEM(populations.shape, f32),
            pltpu.VMEM((4, lz // nx, ly, lx * nx), f32),
        ),
        in_specs=[pl.BlockSpec(memory_space=pl.ANY)],
        out_specs=(pl.BlockSpec(memory_space=pltpu.VMEM),) * 2,
        scratch_shapes=[
            pltpu.VMEM(populations.shape, f32),
            pltpu.VMEM((2, 5) + tile, f32),
            pltpu.VMEM((4,) + tile, f32),
            pltpu.VMEM((2,) + tile, f32),
            pltpu.VMEM((2,) + tile, f32),
            pltpu.VMEM((nx, 2, lx, lz), f32),
            pltpu.VMEM((nx, 2, lx, lz), f32),
            pltpu.VMEM((4, lx * ly, lz), f32),
            pltpu.VMEM((2, 5, lx, lz), f32),
            pltpu.VMEM((2, 5, lx, lz), f32),
            pltpu.VMEM((4, lx, lz), f32),
            pltpu.VMEM((4,) + tile, f32),
            pltpu.SemaphoreType.DMA,
            pltpu.SemaphoreType.DMA((messages,)),
            pltpu.SemaphoreType.DMA((messages,)),
            pltpu.SemaphoreType.DMA((nx,)),
            pltpu.SemaphoreType.DMA((nx,)),
        ],
        compiler_params=pltpu.CompilerParams(collective_id=0, has_side_effects=True),
        name="lattice_step",
    )(populations)
    held = [pltpu.with_memory_space_constraint(h, pltpu.VMEM) for h in held]
    return pl.pallas_call(
        write_out,
        out_shape=tuple(jax.ShapeDtypeStruct(h.shape, f32) for h in held),
        in_specs=[pl.BlockSpec(memory_space=pltpu.VMEM)] * 2,
        out_specs=(pl.BlockSpec(memory_space=pl.ANY),) * 2,
        scratch_shapes=[pltpu.SemaphoreType.DMA((2,))],
        name="write_out",
    )(*held)


def solution(mesh):
    axes = tuple(mesh.axis_names)
    sizes = dict(mesh.shape)
    return jax.shard_map(
        functools.partial(on_device, axes, sizes),
        mesh=mesh,
        in_specs=(P(None, "gx", "gy", "gz"),),
        out_specs=(P(None, "gx", "gy", "gz"), P(None, ("gz", "gx"), "gy", None)),
        check_vma=False,
    )
```

```python
import functools

import jax
import jax.numpy as jnp
from jax import lax
from jax.experimental import pallas as pl
from jax.experimental.pallas import tpu as pltpu
from jax.sharding import PartitionSpec as P

MESH = pl.DeviceIdType.MESH

lattice_moves = [
    (0, 0, 0),
    (1, 0, 0),
    (-1, 0, 0),
    (0, 1, 0),
    (0, -1, 0),
    (0, 0, 1),
    (0, 0, -1),
    (1, 1, 0),
    (-1, -1, 0),
    (1, -1, 0),
    (-1, 1, 0),
    (1, 0, 1),
    (-1, 0, -1),
    (1, 0, -1),
    (-1, 0, 1),
    (0, 1, 1),
    (0, -1, -1),
    (0, 1, -1),
    (0, -1, 1),
]
lattice_weights = [1.0 / 3.0] + [1.0 / 18.0] * 6 + [1.0 / 36.0] * 12
relaxation = 1.6
count_q = len(lattice_moves)


def movers(component, sign):
    return [q for q, move in enumerate(lattice_moves) if move[component] == sign]


def place_in(q, component):
    return movers(component, lattice_moves[q][component]).index(q)


def side(sign):
    return 0 if sign > 0 else 1


edges_xz = [q for q, m in enumerate(lattice_moves) if m[0] and m[2]]
edges_xy = [q for q, m in enumerate(lattice_moves) if m[0] and m[1]]
edges_yz = [q for q, m in enumerate(lattice_moves) if m[1] and m[2]]


def total(terms):
    terms = list(terms)
    while len(terms) > 1:
        terms = [
            terms[i] + terms[i + 1] if i + 1 < len(terms) else terms[i]
            for i in range(0, len(terms), 2)
        ]
    return terms[0]


def moments_of(f):
    density = total(f)
    inverse = 1.0 / density
    velocity = []
    for component in range(3):
        plus = total(f[q] for q in movers(component, 1))
        minus = total(f[q] for q in movers(component, -1))
        velocity.append((plus - minus) * inverse)
    return density, velocity


def collided(f):
    density, velocity = moments_of(f)
    speed_sq = velocity[0] * velocity[0] + velocity[1] * velocity[1] + velocity[2] * velocity[2]
    base = 1.0 - 1.5 * speed_sq
    scaled = {w: (relaxation * w) * density for w in set(lattice_weights)}
    keep = 1.0 - relaxation
    result = [None] * count_q
    result[0] = keep * f[0] + scaled[lattice_weights[0]] * base
    for q in range(1, count_q, 2):
        move = lattice_moves[q]
        projected = None
        for component in range(3):
            if move[component] == 0:
                continue
            if projected is None:
                projected = velocity[component] if move[component] > 0 else -velocity[component]
            elif move[component] > 0:
                projected = projected + velocity[component]
            else:
                projected = projected - velocity[component]
        even = base + 4.5 * (projected * projected)
        odd = 3.0 * projected
        weight = scaled[lattice_weights[q]]
        result[q] = keep * f[q] + weight * (even + odd)
        result[q + 1] = keep * f[q + 1] + weight * (even - odd)
    return result


def rolled(v, shift, axis):
    return pltpu.roll(v, shift % v.shape[axis], axis)


def paired(at, k, n):
    if n & (n - 1):
        return lax.rem(at + k, n)
    bit = 1
    while bit < n:
        if k & bit:
            at = at + bit - 2 * bit * lax.rem(at // bit, 2)
        bit *= 2
    return at


def kernel(axes, sizes, pop_hbm, out_vm, slab_vm,
           pop, face_x, edge_xz, pack_x, pack_z, face_z, send_m, recv_m, mid,
           row_y, face_y, edge_xy, edge_yz,
           load_sem, send_sem, recv_sem, send_m_sem, recv_m_sem):
    nx, ny, nz = (sizes[a] for a in axes)
    here = tuple(lax.axis_index(a) for a in axes)
    _, lx, ly, lz = pop.shape
    split_y = ny > 1

    def device_at(offset):
        return tuple(
            lax.rem(h + (o % n), n) if o % n else h
            for h, o, n in zip(here, offset, (nx, ny, nz))
        )

    offsets = [(k, 0, 0) for k in range(1, nx)]
    offsets += [(0, 0, 1), (0, 0, -1)]
    offsets += [lattice_moves[q] for q in edges_xz]
    if split_y:
        offsets += [(0, 1, 0), (0, -1, 0)]
        offsets += [lattice_moves[q] for q in edges_xy + edges_yz]
    partners = sorted({(a % nx, b % ny, c % nz) for a, b, c in offsets})
    barrier = pltpu.get_barrier_semaphore()
    for offset in partners:
        pl.semaphore_signal(barrier, inc=1, device_id=device_at(offset), device_id_type=MESH)

    load = pltpu.make_async_copy(pop_hbm, pop, load_sem)
    load.start()
    load.wait()

    lane = lax.broadcasted_iota(jnp.int32, (ly, lz), 1)
    row = lax.broadcasted_iota(jnp.int32, (ly, lz), 0)

    for sign in (1, -1):
        at = lz - 1 if sign > 0 else 0
        packed = jnp.zeros((ly, lz), jnp.float32)
        for i, q in enumerate(movers(2, sign)):
            for x in range(lx):
                k = i * lx + x
                packed = jnp.where(lane == k, rolled(pop[q, x], k - at, 1), packed)
        pack_z[side(sign)] = packed
    for sign in (1, -1):
        at = lx - 1 if sign > 0 else 0
        up, down = (lattice_moves.index((sign, 0, cz)) for cz in (1, -1))
        pack_x[side(sign)] = jnp.where(lane == lz - 1, pop[up, at], pop[down, at])
    if split_y:
        for sign in (1, -1):
            at = ly - 1 if sign > 0 else 0
            for i, q in enumerate(movers(1, sign)):
                for x in range(lx):
                    row_y[side(sign), i, x:x + 1, :] = pop[q, x, at:at + 1, :]

    values = [[None] * lx for _ in range(4)]
    for x in range(lx):
        density, velocity = moments_of([pop[q, x] for q in range(count_q)])
        for c, v in enumerate([density] + velocity):
            values[c][x] = v
    for c in range(4):
        tiles = values[c]
        step = 1
        while step < lx:
            upper = (lane & step) != 0
            fresh = list(tiles)
            for x in range(lx):
                if x & step:
                    continue
                a, b = tiles[x], tiles[x + step]
                fresh[x] = jnp.where(upper, rolled(b, step, 1), a)
                fresh[x + step] = jnp.where(upper, b, rolled(a, -step, 1))
            tiles = fresh
            step *= 2
        for z in range(lx):
            mid[c, z * ly:(z + 1) * ly, :] = tiles[z]
    for p in range(2):
        square = mid[2 * p:2 * p + 2].reshape(lz, lz).T
        for j in range(nx):
            send_m[j, p] = square[j * lx:(j + 1) * lx]

    pl.semaphore_wait(barrier, len(partners))

    me = here[0]
    outgoing = []
    count = [0]

    def send(src, dst, offset):
        s = count[0]
        count[0] += 1
        copy = pltpu.make_async_remote_copy(
            src_ref=src, dst_ref=dst, send_sem=send_sem.at[s], recv_sem=recv_sem.at[s],
            device_id=device_at(offset), device_id_type=MESH)
        copy.start()
        outgoing.append(copy)
        return copy

    moment_copies = []

    def send_moments(k):
        target = (paired(here[0], k, nx),) + here[1:]
        copy = pltpu.make_async_remote_copy(
            src_ref=send_m.at[target[0]], dst_ref=recv_m.at[me],
            send_sem=send_m_sem.at[k], recv_sem=recv_m_sem.at[k],
            device_id=target, device_id_type=MESH)
        copy.start()
        moment_copies.append(copy)

    z_copies, x_copies = [], []
    for sign in (1, -1):
        s = side(sign)
        z_copies.append(send(pack_z.at[s], face_z.at[s], (0, 0, sign)))
    for sign in (1, -1):
        s, at = side(sign), lx - 1 if sign > 0 else 0
        for i, q in enumerate(movers(0, sign)):
            x_copies.append(send(pop.at[q, at], face_x.at[s, i], (sign, 0, 0)))
    edge_slot = {}
    for i, q in enumerate(edges_xz):
        cx, _, cz = lattice_moves[q]
        if (cx, cz % nz) not in edge_slot:
            edge_slot[cx, cz % nz] = i
            x_copies.append(send(pack_x.at[side(cx)], edge_xz.at[i], lattice_moves[q]))
    if split_y:
        for sign in (1, -1):
            s = side(sign)
            z_copies.append(send(row_y.at[s], face_y.at[s], (0, sign, 0)))
        for i, q in enumerate(edges_yz):
            s = side(lattice_moves[q][2])
            z_copies.append(send(pack_z.at[s], edge_yz.at[i], lattice_moves[q]))
        for i, q in enumerate(edges_xy):
            s = side(lattice_moves[q][1])
            x_copies.append(send(row_y.at[s, place_in(q, 1)], edge_xy.at[i], lattice_moves[q]))
    order = sorted(range(1, nx), key=lambda k: (k % 2 == 0, -bin(k).count("1"), abs(k - 11)))
    early = [k for k in order if bin(k).count("1") > 2]
    order = early + [k for k in order if k not in early]
    for k in early:
        send_moments(k)
    for k in order[len(early):]:
        send_moments(k)
    recv_m[me] = send_m[me]

    def streamed(q, x):
        cx, cy, cz = lattice_moves[q]
        sx = x - cx
        inside = 0 <= sx < lx
        sx_wrapped = sx % lx
        v = pop[q, sx] if inside else face_x[side(cx), place_in(q, 0)]
        if cy and split_y:
            at = ly - 1 if cy > 0 else 0
            if inside:
                other = face_y[side(cy), place_in(q, 1), sx:sx + 1, :]
            else:
                other = edge_xy[edges_xy.index(q), sx_wrapped:sx_wrapped + 1, :]
            v = jnp.where(row == at, jnp.broadcast_to(other, v.shape), v)
        if cz:
            at = lz - 1 if cz > 0 else 0
            if inside:
                other = face_z[side(cz)]
                if cy and split_y:
                    at_y = ly - 1 if cy > 0 else 0
                    other = jnp.where(row == at_y, edge_yz[edges_yz.index(q)], other)
                k = place_in(q, 2) * lx + sx
                other = rolled(other, at - k, 1)
            else:
                other = edge_xz[edge_slot[cx, cz % nz]]
            v = jnp.where(lane == at, other, v)
        if cy:
            v = rolled(v, cy, 0)
        if cz:
            v = rolled(v, cz, 1)
        return v

    def advance(x):
        result = collided([streamed(q, x) for q in range(count_q)])
        for q in range(count_q):
            out_vm[q, x] = result[q]

    for copy in z_copies:
        copy.wait_recv()
    for x in range(1, lx - 1):
        advance(x)
    for copy in x_copies:
        copy.wait_recv()
    advance(0)
    advance(lx - 1)

    for copy in moment_copies:
        copy.wait_recv()
    for p in range(2):
        square = recv_m[:, p].reshape(lz, lz).T
        slab_vm[2 * p:2 * p + 2] = square.reshape(2, lx, ly, lz)
    for copy in outgoing + moment_copies:
        copy.wait_send()


def write_out(next_vm, slab_vm, next_ref, slab_ref, sems):
    stores = [
        pltpu.make_async_copy(next_vm, next_ref, sems.at[0]),
        pltpu.make_async_copy(slab_vm, slab_ref, sems.at[1]),
    ]
    for store in stores:
        store.start()
    for store in stores:
        store.wait()


def on_device(axes, sizes, populations):
    q, lx, ly, lz = populations.shape
    nx = sizes[axes[0]]
    messages = 2 + 10 + 4
    if sizes[axes[1]] > 1:
        messages += 2 + 4 + 4
    f32 = jnp.float32
    tile = (ly, lz)
    held = pl.pallas_call(
        functools.partial(kernel, axes, sizes),
        out_shape=(
            pltpu.VMEM(populations.shape, f32),
            pltpu.VMEM((4, lz // nx, ly, lx * nx), f32),
        ),
        in_specs=[pl.BlockSpec(memory_space=pl.ANY)],
        out_specs=(pl.BlockSpec(memory_space=pltpu.VMEM),) * 2,
        scratch_shapes=[
            pltpu.VMEM(populations.shape, f32),
            pltpu.VMEM((2, 5) + tile, f32),
            pltpu.VMEM((4,) + tile, f32),
            pltpu.VMEM((2,) + tile, f32),
            pltpu.VMEM((2,) + tile, f32),
            pltpu.VMEM((2,) + tile, f32),
            pltpu.VMEM((nx, 2, lx, lz), f32),
            pltpu.VMEM((nx, 2, lx, lz), f32),
            pltpu.VMEM((4, lx * ly, lz), f32),
            pltpu.VMEM((2, 5, lx, lz), f32),
            pltpu.VMEM((2, 5, lx, lz), f32),
            pltpu.VMEM((4, lx, lz), f32),
            pltpu.VMEM((4,) + tile, f32),
            pltpu.SemaphoreType.DMA,
            pltpu.SemaphoreType.DMA((messages,)),
            pltpu.SemaphoreType.DMA((messages,)),
            pltpu.SemaphoreType.DMA((nx,)),
            pltpu.SemaphoreType.DMA((nx,)),
        ],
        compiler_params=pltpu.CompilerParams(collective_id=0, has_side_effects=True),
        name="lattice_step",
    )(populations)
    held = [pltpu.with_memory_space_constraint(h, pltpu.VMEM) for h in held]
    return pl.pallas_call(
        write_out,
        out_shape=tuple(jax.ShapeDtypeStruct(h.shape, f32) for h in held),
        in_specs=[pl.BlockSpec(memory_space=pltpu.VMEM)] * 2,
        out_specs=(pl.BlockSpec(memory_space=pl.ANY),) * 2,
        scratch_shapes=[pltpu.SemaphoreType.DMA((2,))],
        name="write_out",
    )(*held)


def solution(mesh):
    axes = tuple(mesh.axis_names)
    sizes = dict(mesh.shape)
    return jax.shard_map(
        functools.partial(on_device, axes, sizes),
        mesh=mesh,
        in_specs=(P(None, "gx", "gy", "gz"),),
        out_specs=(P(None, "gx", "gy", "gz"), P(None, ("gz", "gx"), "gy", None)),
        check_vma=False,
    )
```
